32 devices in a mesh: dp: 2 (over y), expert: 4 (over z), ffn: 4 (over x, core).
Axes of the slice: x: 2, y: 2, z: 4, core: 2. Of those that a mesh axis runs over, the one named last changes fastest.
Arguments:
- tokens: bfloat16 [64, 6144], P(('dp', 'expert'), 'ffn'), may hold values from -6 to 6
- out_grad: bfloat16 [64, 6144], P(('dp', 'expert'), 'ffn'), may hold values from -6 to 6
- expert_ids: int32 [64, 2], P(('dp', 'expert')), may hold values from 0 to 3, all different within a row; in each aligned block of 8 rows (0 to 7, 8 to 15, ...) at most 6 rows name the same one
- tenant_ids: int32 [64], P(('dp', 'expert')), may hold values from 0 to 7
- router_logits: float32 [64, 2], P(('dp', 'expert')), may hold values from -8 to 8
- gate_projection_weight: bfloat16 [4, 6144, 8192], P('expert', None, ('dp', 'ffn')), may hold values from -0.078125 to 0.078125
- up_projection_weight: bfloat16 [4, 6144, 8192], P('expert', None, ('dp', 'ffn')), may hold values from -0.078125 to 0.078125
- down_projection_weight: bfloat16 [4, 8192, 6144], P('expert', ('dp', 'ffn')), may hold values from -0.0625 to 0.0625
- input_down_maps: bfloat16 [4, 6144, 256], P('expert', 'ffn'), may hold values from -0.078125 to 0.078125
- input_up_maps: bfloat16 [4, 2, 128, 8192], P('expert', None, None, ('dp', 'ffn')), may hold values from -1.5 to 1.5
- output_down_map: bfloat16 [4, 8192, 128], P('expert', ('dp', 'ffn')), may hold values from -0.0625 to 0.0625
- output_up_map: bfloat16 [4, 128, 6144], P('expert', None, 'ffn'), may hold values from -1.5 to 1.5
Outputs:
- mixed: bfloat16 [64, 6144], P(('dp', 'expert'), 'ffn')
- input_grad: bfloat16 [64, 6144], P(('dp', 'expert'), 'ffn')
- input_down_gradient: float32 [4, 6144, 256], P('expert', 'ffn')
- input_up_gradient: float32 [4, 2, 128, 8192], P('expert', None, None, ('dp', 'ffn'))
- output_down_gradient: float32 [4, 8192, 128], P('expert', ('dp', 'ffn'))
- output_up_gradient: float32 [4, 128, 6144], P('expert', None, 'ffn')
The draws below stay inside these ranges and needn't reach their ends.
Inputs may be any that keep to these rules, and one draw needn't show every extreme that they name: `expert_ids`: each row names 2 different experts. Among the rows of one device's block of 8 tokens no expert is named more than 6 times; in some blocks one expert is named exactly 6 times.
All inputs are finite; a program needn't handle non-finite values.
Results may differ from the reference program's by a relative error of at most 0.0073.
Values may be sent and summed in bfloat16 or wider, within the bound.
A program may use at most 256 MiB of HBM per device.

```python
import math
import jax
import jax.numpy as jnp
import numpy as np
from jax import lax

D = 6144
FF = 8192
RANK = 16
TENANTS = 8
TOP = 2
TOK_DEV = 8
EXPERTS = 4
TOKENS = 64
CAP = 6
ROWS = 48
TENANT_RANKS = 128


def touch_ends(drawn, stream_key, low, largest):
    place = [jax.random.randint(jax.random.fold_in(stream_key, axis), (), 0, length) for axis, length in enumerate(drawn.shape)]
    main_axis = drawn.shape.index(max(drawn.shape))
    next_to = place[:main_axis] + [(place[main_axis] + 1) % drawn.shape[main_axis]] + place[main_axis + 1:]
    return drawn.at[tuple(place)].set(low).at[tuple(next_to)].set(largest)


def block_levels(key, dims, split, least, high):
    factor_of = 1.0
    for dim, shards_of in split:
        heights = jax.random.uniform(jax.random.fold_in(jax.random.fold_in(key, 6), dim), (shards_of,), jnp.float32, least / len(split), high / len(split))
        factor_of = factor_of * jnp.repeat(jnp.exp(heights), dims[dim] // shards_of).reshape((-1,) + (1,) * (len(dims) - 1 - dim))
    return factor_of


def routed_block(stream_key, own, number, rows, number_of, top, limit, lean):
    order = jax.random.permutation(stream_key, number_of)
    heavy_load, ordinary = shares(number_of, rows * top, limit, lean, True), shares(number_of, rows * top, limit, lean, False)
    places = jnp.arange(number_of)

    def named(tallies, offset_by):
        used = int((tallies > 0).sum())
        fixed = max(1, used // 4)
        shifted = fixed + (places - fixed + offset_by * (used - fixed)) % max(1, number_of - fixed)
        return jnp.zeros((number_of,), jnp.int32).at[order[jnp.where(places < fixed, places, shifted)]].set(jnp.asarray(tallies, jnp.int32))

    tallies = jnp.where(number % 4 == 0, named(heavy_load, number // 4), named(ordinary, number - number // 4 - 1))
    mixed = jax.random.permutation(jax.random.fold_in(own, 3), number_of)
    source_of, sink = mixed[0:number_of // 2 * 2:2], mixed[1:number_of // 2 * 2:2]
    margin = jnp.minimum(tallies[source_of] - 1, limit - tallies[sink]) // 2
    margin = jnp.where((source_of == order[0]) | (sink == order[0]) | (tallies[sink] == 0), 0, jnp.maximum(margin, 0))
    shifted = jax.random.randint(jax.random.fold_in(own, 4), (number_of // 2,), 0, 1 << 20) % (margin + 1)
    tallies = tallies.at[source_of].add(-shifted).at[sink].add(shifted)
    members = jnp.searchsorted(jnp.cumsum(tallies), jnp.arange(rows * top), side="right").astype(jnp.int32)
    table = members.reshape(top, rows).T
    table = table[jax.random.permutation(jax.random.fold_in(own, 1), rows)]
    offset_by = jax.random.randint(jax.random.fold_in(own, 2), (rows, 1), 0, top)
    return jnp.take_along_axis(table, (jnp.arange(top)[None, :] + offset_by) % top, axis=1)


def shares(count, total, most, skew, full):
    weights = [(1 << 20) // math.isqrt(grade ** skew) + 1 for grade in range(1, count + 1)]
    largest = most if full else min(most, max(-(-total // count), total * weights[0] // sum(weights)))
    least = 1 if total - largest >= count - 1 else 0
    given, rest = [largest] + [least] * (count - 1), total - largest - least * (count - 1)
    while rest > 0:
        candidates = [i for i in range(1, count) if given[i] < largest] or [i for i in range(1, count) if given[i] < most]
        mass, remaining = sum([weights[i] for i in candidates]), rest
        for i in candidates:
            extra = min(most - given[i], max(1, remaining * weights[i] // mass), rest)
            given[i] = given[i] + extra
            rest = rest - extra
    return np.array(given)


def scatter_about(own_key, dims, deviation, reach, shards=(), kind=jnp.bfloat16):
    entries = deviation * jax.random.normal(own_key, dims, jnp.float32)
    if shards:
        entries = entries * block_levels(own_key, dims, shards, -0.22, 0.18)
    return jnp.clip(entries, -reach, reach).astype(kind)


def setup_inputs(seed: int = 0) -> dict:
    keys = jax.random.split(jax.random.key(seed), 13)
    tokens = scatter_about(keys[0], (TOKENS, D), 1.0, 6.0, ((0, 8), (1, 4)))
    out_grad = scatter_about(keys[1], (TOKENS, D), 1.0, 6.0, ((0, 8), (1, 4)))
    expert_ids_keys = jax.random.split(jax.random.fold_in(keys[2], 1), TOKENS // TOK_DEV)
    expert_ids_turns = jax.random.permutation(jax.random.fold_in(keys[2], 3), TOKENS // TOK_DEV)
    expert_ids = jax.vmap(lambda own, number: routed_block(jax.random.fold_in(keys[2], 2), own, number, TOK_DEV, EXPERTS, TOP, CAP, 2))(expert_ids_keys, expert_ids_turns).reshape((TOKENS, TOP))
    tenant_ids = touch_ends(jax.random.randint(keys[3], (TOKENS,), 0, TENANTS), jax.random.fold_in(keys[3], 1), 0, TENANTS - 1).astype(jnp.int32)
    router_logits = scatter_about(keys[4], (TOKENS, TOP), 1.5, 8.0, ((0, 8),), jnp.float32)
    gate_projection_weight = scatter_about(keys[5], (EXPERTS, D, FF), D ** -0.5, 0.078125, ((0, 4), (2, 8)))
    up_projection_weight = scatter_about(keys[6], (EXPERTS, D, FF), D ** -0.5, 0.078125, ((0, 4), (2, 8)))
    down_projection_weight = scatter_about(keys[7], (EXPERTS, FF, D), FF ** -0.5, 0.0625, ((0, 4), (1, 8)))
    input_down_maps = scatter_about(keys[8], (EXPERTS, D, 2 * TENANT_RANKS), D ** -0.5, 0.078125, ((0, 4), (1, 4)))
    input_up_maps = scatter_about(keys[9], (EXPERTS, 2, TENANT_RANKS, FF), RANK ** -0.5, 1.5, ((0, 4), (3, 8)))
    output_down_map = scatter_about(keys[10], (EXPERTS, FF, TENANT_RANKS), FF ** -0.5, 0.0625, ((0, 4), (1, 8)))
    output_up_map = scatter_about(keys[11], (EXPERTS, TENANT_RANKS, D), RANK ** -0.5, 1.5, ((0, 4), (2, 4)))
    return {"tokens": tokens, "out_grad": out_grad, "expert_ids": expert_ids, "tenant_ids": tenant_ids, "router_logits": router_logits, "gate_projection_weight": gate_projection_weight, "up_projection_weight": up_projection_weight, "down_projection_weight": down_projection_weight, "input_down_maps": input_down_maps, "input_up_maps": input_up_maps, "output_down_map": output_down_map, "output_up_map": output_up_map}


ADAPTER_SCALE = 0.5


def matrix_product(left, right):
    return jnp.dot(left, right, preferred_element_type=jnp.float32)


def slot_rows(expert_ids):
    blocked = expert_ids.reshape(-1, TOK_DEV * TOP)
    labels = jnp.arange(EXPERTS, dtype=jnp.int32)
    onehot = (blocked[:, :, None] == labels[None, None, :]).astype(jnp.int32)
    before = jnp.cumsum(onehot, axis=1) - onehot
    position = jnp.sum(before * onehot, axis=2).astype(jnp.int32)
    block_index = jnp.arange(blocked.shape[0], dtype=jnp.int32)[:, None]
    return (block_index * CAP + position).reshape(-1, TOP).astype(jnp.int32)


def expert_step(inputs):
    (expert_token_rows, expert_gradients, exp_tenant, gate_matrix, up_matrix, down_matrix,
     expert_input_down, expert_input_up, expert_output_down, expert_output_up) = inputs
    columns = jnp.arange(TENANT_RANKS, dtype=jnp.int32) // RANK
    tenant_column_mask = (exp_tenant[:, None] == columns[None, :]).astype(jnp.float32)
    paired_mask = jnp.concatenate([tenant_column_mask, tenant_column_mask], axis=1)
    adapter_input = matrix_product(expert_token_rows, expert_input_down)
    adapter_rows = (paired_mask * adapter_input).astype(jnp.bfloat16)
    gate_activation = matrix_product(expert_token_rows, gate_matrix) + ADAPTER_SCALE * matrix_product(adapter_rows[:, :TENANT_RANKS], expert_input_up[0])
    up_activation = matrix_product(expert_token_rows, up_matrix) + ADAPTER_SCALE * matrix_product(adapter_rows[:, TENANT_RANKS:], expert_input_up[1])
    activated = jax.nn.silu(gate_activation)
    hidden_state = (activated * up_activation).astype(jnp.bfloat16)
    down_adapter_term = matrix_product(hidden_state, expert_output_down)
    down_row_values = (tenant_column_mask * down_adapter_term).astype(jnp.bfloat16)
    expert_output = (matrix_product(hidden_state, down_matrix) + ADAPTER_SCALE * matrix_product(down_row_values, expert_output_up)).astype(jnp.bfloat16)
    adapter_backward = matrix_product(expert_gradients, expert_output_up.T)
    backward_rows = (tenant_column_mask * adapter_backward).astype(jnp.bfloat16)
    hidden_gradient = matrix_product(expert_gradients, down_matrix.T) + ADAPTER_SCALE * matrix_product(backward_rows, expert_output_down.T)
    output_down_gradient = ADAPTER_SCALE * matrix_product(hidden_state.T, backward_rows)
    output_up_gradient = ADAPTER_SCALE * matrix_product(down_row_values.T, expert_gradients)
    sigmoid_gate = jax.nn.sigmoid(gate_activation)
    gate_gradient = (hidden_gradient * up_activation * sigmoid_gate * (1.0 + gate_activation * (1.0 - sigmoid_gate))).astype(jnp.bfloat16)
    up_gradient = (hidden_gradient * activated).astype(jnp.bfloat16)
    input_up_gradient = ADAPTER_SCALE * jnp.stack([matrix_product(adapter_rows[:, :TENANT_RANKS].T, gate_gradient), matrix_product(adapter_rows[:, TENANT_RANKS:].T, up_gradient)])
    up_adapter_term = jnp.concatenate([matrix_product(gate_gradient, expert_input_up[0].T), matrix_product(up_gradient, expert_input_up[1].T)], axis=1)
    up_row_values = (paired_mask * up_adapter_term).astype(jnp.bfloat16)
    input_down_gradient = ADAPTER_SCALE * matrix_product(expert_token_rows.T, up_row_values)
    running_partial_sum = matrix_product(gate_gradient, gate_matrix.T) + matrix_product(up_gradient, up_matrix.T)
    input_result = (running_partial_sum + ADAPTER_SCALE * matrix_product(up_row_values, expert_input_down.T)).astype(jnp.bfloat16)
    return expert_output, input_result, input_down_gradient, input_up_gradient, output_down_gradient, output_up_gradient


def reference(tokens, out_grad, expert_ids, tenant_ids, router_logits, gate_projection_weight, up_projection_weight, down_projection_weight, input_down_maps, input_up_maps, output_down_map, output_up_map):
    slot_index = slot_rows(expert_ids)
    flat_index = (expert_ids * ROWS + slot_index).reshape(-1).astype(jnp.int32)
    prob_first = jax.nn.sigmoid(router_logits[:, 0] - router_logits[:, 1])
    gate_probs = jnp.stack([prob_first, 1.0 - prob_first], axis=1)
    total_rows = EXPERTS * ROWS
    token_copies = jnp.repeat(tokens, TOP, axis=0)
    grad_copies = (gate_probs[:, :, None] * out_grad.astype(jnp.float32)[:, None, :]).astype(jnp.bfloat16).reshape(-1, D)
    tenant_copies = jnp.repeat(tenant_ids, TOP).astype(jnp.int32)
    expert_token_rows = jnp.zeros((total_rows, D), jnp.bfloat16).at[flat_index].set(token_copies)
    expert_gradients = jnp.zeros((total_rows, D), jnp.bfloat16).at[flat_index].set(grad_copies)
    exp_tenant = jnp.full((total_rows,), -1, jnp.int32).at[flat_index].set(tenant_copies)
    results = lax.map(expert_step, (expert_token_rows.reshape(EXPERTS, ROWS, D), expert_gradients.reshape(EXPERTS, ROWS, D),
                                    exp_tenant.reshape(EXPERTS, ROWS), gate_projection_weight, up_projection_weight, down_projection_weight, input_down_maps, input_up_maps, output_down_map, output_up_map))
    expert_output, input_result, input_down_gradient, input_up_gradient, output_down_gradient, output_up_gradient = results
    out_picked = expert_output.reshape(total_rows, D).astype(jnp.float32)[flat_index].reshape(-1, TOP, D)
    mixed = jnp.sum(gate_probs[:, :, None] * out_picked, axis=1).astype(jnp.bfloat16)
    grad_picked = input_result.reshape(total_rows, D).astype(jnp.float32)[flat_index].reshape(-1, TOP, D)
    input_grad = jnp.sum(grad_picked, axis=1).astype(jnp.bfloat16)
    return mixed, input_grad, input_down_gradient, input_up_gradient, output_down_gradient, output_up_gradient
```

```python
import functools

import jax
import jax.numpy as jnp
from jax import lax
from jax.experimental import pallas as pl
from jax.experimental.pallas import tpu as pltpu
from jax.sharding import PartitionSpec as P

RANK = 16
SCALE = 0.5
F32 = jnp.float32
BF16 = jnp.bfloat16
HIGH = lax.Precision.HIGHEST
LANES = 128


def dot(a, b, dims=((1,), (0,)), precision=None):
    return lax.dot_general(
        a, b, (dims, ((), ())), preferred_element_type=F32, precision=precision
    )


def dot_nt(a, b, precision=None):
    return dot(a, b, ((1,), (1,)), precision)


def dot_tn(a, b):
    return dot(a, b, ((0,), (0,)))


def flip(index, mask):
    bit = 1
    while bit <= mask:
        if mask & bit:
            index = index + bit - 2 * bit * ((index // bit) % 2)
        bit *= 2
    return index


def bits_of(size):
    assert size & (size - 1) == 0
    return [1 << i for i in range(size.bit_length() - 1)]


def orders(nd, nf):
    fb = [("f", b) for b in reversed(bits_of(nf))]
    db = [("d", b) for b in reversed(bits_of(nd))]
    core = fb[-1:]
    return (fb[:-1] + db + core, db + fb[:-1] + core)


def stages(dims, mask):
    return [i for i, (a, b) in enumerate(dims) if mask[0 if a == "f" else 1] & b]


def step(mask, dim):
    a, b = dim
    return (mask[0] ^ b, mask[1]) if a == "f" else (mask[0], mask[1] ^ b)


def all_masks(nd, nf):
    return [(mf, r) for mf in range(nf) for r in range(nd)]


def received(dims, i, nd, nf):
    return [m for m in all_masks(nd, nf) if all(j > i for j in stages(dims, m))]


def layer_kernel(
    nd, ne, nf, tok,
    tokens, out_grad, ids, tids, logits, wg_hbm, wu_hbm, wd_hbm, idm_hbm, iup_hbm, odm_hbm, oum_hbm,
    mixed, igrad, idg, iug, odg, oug,
    tok_v, grad_v, ids_v, tids_v, logits_v, idm, iup, odm, oum,
    src, msrc, wts, held, masks, wg, wu, wd, gate, up, dh, hid, dgr, dur,
    part, rcore, back, home, ar1s, ar1r, ar2s, ar2r, *rest,
):
    routes = orders(nd, nf)
    core = routes[0][-1]
    rsd = [[core] + [x for x in r if x != core] for r in routes]
    rbuf = {}
    n = 0
    for h in range(2):
        for i in range(1, len(rsd[h])):
            rbuf[h, i] = rest[n]
            n += 1
    isem, wsem, ssem, rsem = rest[n:]
    d, e, f = lax.axis_index("dp"), lax.axis_index("expert"), lax.axis_index("ffn")
    quarter = tokens.shape[1]
    hidden = gate.shape[1]
    rows_d = ne * tok
    rows = nd * rows_d
    half = quarter // 2
    ntr = odm.shape[1]
    pending = []
    counter = [0]

    def peer(dim):
        a, b = dim
        return (d, e, flip(f, b)) if a == "f" else (flip(d, b), e, f)

    def send(s, t, dev):
        i = counter[0]
        counter[0] += 1
        c = pltpu.make_async_remote_copy(
            src_ref=s, dst_ref=t, send_sem=ssem.at[i], recv_sem=rsem.at[i],
            device_id=dev, device_id_type=pl.DeviceIdType.MESH,
        )
        c.start()
        pending.append(c)
        return c

    barrier = pltpu.get_barrier_semaphore()
    peers = [(d, flip(e, m), f) for m in range(1, ne)] + [peer(x) for x in routes[0]]
    for p in peers:
        pl.semaphore_signal(barrier, inc=1, device_id=p, device_id_type=pl.DeviceIdType.MESH)

    def load(s, t, sem):
        c = pltpu.make_async_copy(s, t, sem)
        c.start()
        return c

    first = [
        load(a, b, isem.at[i])
        for i, (a, b) in enumerate(
            [(ids, ids_v), (tids, tids_v), (logits, logits_v), (tokens, tok_v), (out_grad, grad_v)]
        )
    ]
    for c in first:
        c.wait()
    maps = [
        load(a, b, isem.at[5 + i])
        for i, (a, b) in enumerate(
            [(idm_hbm.at[0], idm), (oum_hbm.at[0], oum), (iup_hbm.at[0], iup), (odm_hbm.at[0], odm)]
        )
    ]
    wcopies = {}
    for m in range(nf):
        at = pl.ds(pl.multiple_of(flip(f, m) * quarter, LANES), quarter)
        wcopies[m] = [
            load(wg_hbm.at[0, at, :], wg.at[m], wsem.at[3 * m]),
            load(wu_hbm.at[0, at, :], wu.at[m], wsem.at[3 * m + 1]),
            load(wd_hbm.at[0, :, at], wd.at[m], wsem.at[3 * m + 2]),
        ]

    eye = lax.broadcasted_iota(jnp.int32, (tok, tok), 0) == lax.broadcasted_iota(jnp.int32, (tok, tok), 1)

    def upright(row):
        return jnp.sum(jnp.where(eye, jnp.broadcast_to(row, (tok, tok)), 0.0), axis=1, keepdims=True)

    lg = logits_v[...]
    p0 = jax.nn.sigmoid(upright(lg[0:1]) - upright(lg[1:2]))
    idv = ids_v[...].astype(F32)
    choice = (upright(idv[0:1]), upright(idv[1:2]))
    tcol = upright(tids_v[...].astype(F32))
    column = (lax.broadcasted_iota(jnp.int32, (tok, ntr), 1) // RANK).astype(F32)
    tmask = (tcol == column).astype(F32)
    tv = tok_v[...].astype(F32)
    gv = grad_v[...].astype(F32)
    for k in range(ne):
        hit = [(c == float(k)).astype(F32) for c in choice]
        member = hit[0] + hit[1]
        weight = hit[0] * p0 + hit[1] * (1.0 - p0)
        src[k, 0] = (tv * member).astype(BF16)
        src[k, 1] = (gv * weight).astype(BF16)
        msrc[k] = tmask * member
        wts[k] = jnp.broadcast_to(weight, (tok, LANES))
    pl.semaphore_wait(barrier, len(peers))

    def block(mf, r, lo, n):
        return held.at[mf, :, pl.ds(r * rows_d + lo * tok, n * tok), :]

    zc = {}
    zm = {}
    for m in range(1, ne):
        to = (d, flip(e, m), f)
        zc[m] = send(src.at[flip(e, m)], block(0, 0, m, 1), to)
    for m in range(1, ne):
        to = (d, flip(e, m), f)
        zm[m] = send(msrc.at[flip(e, m)], masks.at[0, pl.ds(m * tok, tok), :], to)

    arrivals = {}
    hn = max(ne // 2, 1)

    def forward(s, mask, route, lo, n):
        dims = routes[route]
        last = max(stages(dims, mask), default=-1)
        for i in range(last + 1, len(dims)):
            to = step(mask, dims[i])
            c = send(s, block(to[0], to[1], lo, n), peer(dims[i]))
            arrivals.setdefault((to, route), []).append((lo, n, c))

    held[0, :, pl.ds(0, tok), :] = src[e]
    masks[0, pl.ds(0, tok), :] = msrc[e]
    forward(src.at[e], (0, 0), 0, 0, 1)
    znear = [1] + [m for m in range(ne - 1, 1, -1)] if ne > 1 else []
    for m in znear:
        zc[m].wait_recv()
        forward(block(0, 0, m, 1), (0, 0), m // hn, m, 1)

    def pass_on(mask, route):
        for lo, n, c in arrivals[mask, route]:
            c.wait_recv()
            if n == 1 and ne > 4:
                continue
            forward(block(mask[0], mask[1], lo, n), mask, route, lo, n)
        if ne > 4 and arrivals[mask, route][0][1] == 1:
            forward(block(mask[0], mask[1], route * hn, hn), mask, route, route * hn, hn)

    def by_last(mask):
        return [max(stages(routes[h], mask)) for h in range(2)]

    for m in range(1, ne):
        zm[m].wait_recv()
    mc = []
    have = [0]
    for a, b in [x for x in routes[0] if x[0] == "d"]:
        got = [send(masks.at[r], masks.at[r ^ b], peer((a, b))) for r in have]
        mc.append(got)
        have = have + [r ^ b for r in have]
        if len(mc) < len(bits_of(nd)):
            for c in got:
                c.wait_recv()

    todo = [(m, h) for m in all_masks(nd, nf) if m != (0, 0) for h in range(2)]
    todo = [(m, h) for m, h in todo if stages(routes[h], m)[-1] != len(routes[h]) - 1]
    todo.sort(key=lambda t: (len(stages(routes[t[1]], t[0])), stages(routes[t[1]], t[0])[-1]))
    done = set()

    def run_until(need):
        while todo and not all(t in done for t in need):
            m, h = todo.pop(0)
            pass_on(m, h)
            done.add((m, h))

    run_until([((0, r), h) for r in range(1, nd) for h in range(2)])
    for got in mc[-1:]:
        for c in got:
            c.wait_recv()
    for c in maps:
        c.wait()

    mask = masks[...].reshape(rows, ntr)
    mask3 = jnp.concatenate([mask, mask, mask], axis=1)
    col = lax.broadcasted_iota(jnp.int32, (3 * ntr, LANES), 0)
    lane = lax.broadcasted_iota(jnp.int32, (3 * ntr, LANES), 1)
    select = ((col // ntr) * RANK + col % RANK == lane).astype(F32)

    def compress(v):
        return dot(v * mask3, select, precision=HIGH)

    def expand(v):
        return dot_nt(v, select, precision=HIGH) * mask3

    def all_reduce(v, dims, sbuf, rbuf):
        for i, dim in enumerate(dims):
            sbuf[i] = v
            c = send(sbuf.at[i], rbuf.at[i], peer(dim))
            yield None
            c.wait_recv()
            got = rbuf[i]
            if dim[0] == "d":
                got = jnp.concatenate(
                    [got[(r ^ dim[1]) * rows_d : ((r ^ dim[1]) + 1) * rows_d] for r in range(nd)], axis=0
                )
            v = v + got
        yield v

    pv = jnp.concatenate([dot(held[0, 0], idm[...]), dot_nt(held[0, 1], oum[...])], axis=1)
    ar1 = all_reduce(compress(pv), [x for x in routes[0] if x[0] == "f"], ar1s, ar1r)
    next(ar1)

    def project(m, start):
        for c in wcopies[m]:
            c.wait()
        x, y = held[m, 0], held[m, 1]
        g, u, h = dot(x, wg[m]), dot(x, wu[m]), dot_nt(y, wd[m])
        if start:
            gate[...] = g
            up[...] = u
            dh[...] = h
        else:
            gate[...] += g
            up[...] += u
            dh[...] += h

    project(0, True)
    run_until([t for t in todo])
    pv = next(ar1)
    for m in range(1, nf):
        for r in range(nd):
            for h in range(2):
                if max(stages(routes[h], (m, r))) == len(routes[h]) - 1:
                    for _, _, c in arrivals[(m, r), h]:
                        c.wait_recv()
        project(m, False)
        if pv is None:
            pv = next(ar1)
    while pv is None:
        pv = next(ar1)
    pv = expand(pv)
    q = pv[:, : 2 * ntr].astype(BF16)
    vq = pv[:, 2 * ntr :].astype(BF16)

    aw = min(hidden, 256 if rows <= 64 else 128)
    for k in range(hidden // aw):
        at = slice(k * aw, (k + 1) * aw)
        g = gate[:, at] + SCALE * dot(q[:, :ntr], iup[0, :, at])
        u = up[:, at] + SCALE * dot(q[:, ntr:], iup[1, :, at])
        t = dh[:, at] + SCALE * dot_nt(vq, odm[at, :])
        s = jax.nn.sigmoid(g)
        gs = g * s
        hid[:, at] = (gs * u).astype(BF16)
        dgr[:, at] = (t * u * s * (1.0 + g * (1.0 - s))).astype(BF16)
        dur[:, at] = (t * gs).astype(BF16)

    z = dot(hid[...], odm[...])
    w0 = dot_nt(dgr[...], iup[0])
    w1 = dot_nt(dur[...], iup[1])
    ar2 = all_reduce(
        compress(jnp.concatenate([z, w0, w1], axis=1)), list(reversed(routes[0])), ar2s, ar2r
    )
    next(ar2)

    rec = {}

    def cols(h):
        return pl.ds(h * half, half)

    def rowsof(r):
        return pl.ds(r * rows_d, rows_d)

    def produce(k, m):
        if k == 0:
            v = dot(hid[...], wd[m])
        else:
            v = dot_nt(dgr[...], wg[m]) + dot_nt(dur[...], wu[m])
        part[k, m] = v.astype(BF16)
        if m & core[1]:
            rec[k, m ^ core[1]] = send(
                part.at[k, m], rcore.at[k, received_core.index(m ^ core[1])], peer(core)
            )

    received_core = [m for m in range(nf) if not m & core[1]]

    def add_core(k, m):
        rec[k, m].wait_recv()
        part[k, m] = (part[k, m].astype(F32) + rcore[k, received_core.index(m)].astype(F32)).astype(BF16)

    def pieces(k, h, i, only):
        dims = rsd[h]
        for m in all_masks(nd, nf):
            st = stages(dims, m)
            if st and st[0] == i and only(m):
                for j in range(1, i):
                    take(k, h, j, m)
                to = step(m, dims[i])
                slot = received(dims, i, nd, nf).index(to)
                rec[k, h, i, to] = send(
                    part.at[k, m[0], rowsof(m[1]), cols(h)], rbuf[h, i].at[k, slot], peer(dims[i])
                )

    def take(k, h, j, m):
        rec[k, h, j, m].wait_recv()
        slot = received(rsd[h], j, nd, nf).index(m)
        at = (k, m[0], rowsof(m[1]), cols(h))
        part[at] = (part[at].astype(F32) + rbuf[h, j][k, slot].astype(F32)).astype(BF16)

    zret = {}

    def finish(k, h, extra):
        dims = rsd[h]
        total = part[k, 0, rowsof(0), cols(h)].astype(F32)
        for j in range(1, len(dims)):
            rec[k, h, j, (0, 0)].wait_recv()
            slot = received(dims, j, nd, nf).index((0, 0))
            total = total + rbuf[h, j][k, slot].astype(F32)
        total = total + extra[:, h * half : (h + 1) * half]
        back[k, :, cols(h)] = total.astype(BF16)
        for m in range(1, ne):
            zret[k, h, m] = send(
                back.at[k, pl.ds(m * tok, tok), cols(h)], home.at[k, m, :, cols(h)], (d, flip(e, m), f)
            )

    order = sorted(range(nf), key=lambda m: (-(m & ~core[1]), not m & core[1]))
    for m in order:
        produce(0, m)

    def stage_of(k, i):
        for h in range(2):
            pieces(k, h, i, lambda m: True)

    nst = len(rsd[0])
    produce(1, order[0])
    for m in received_core:
        add_core(0, m)
    stage_of(0, 1)
    zw = next(ar2)
    mid = order[1:-1]
    later = list(range(2, nst))
    early1 = [m for m in received_core if m != order[-1]]
    for n, m in enumerate(mid):
        produce(1, m)
        if zw is None:
            zw = next(ar2)
        if m in early1:
            add_core(1, m)
            for h in range(2):
                pieces(1, h, 1, lambda t, m=m: t[0] == m)
        if later:
            stage_of(0, later.pop(0))
    while later:
        stage_of(0, later.pop(0))
    while zw is None:
        zw = next(ar2)
    zw = expand(zw)
    qz = zw[:, :ntr].astype(BF16)
    wq = zw[:, ntr:].astype(BF16)
    y_add = SCALE * dot(qz[:rows_d], oum[...])
    for h in range(2):
        finish(0, h, y_add)
    produce(1, order[-1])
    add_core(1, order[-1])
    for h in range(2):
        pieces(1, h, 1, lambda t: t[0] == order[-1])
    x_add = SCALE * dot_nt(wq[:rows_d], idm[...])
    for i in range(2, nst):
        stage_of(1, i)
    odg[...] = SCALE * dot_tn(hid[...], vq)
    iug[0] = SCALE * dot_tn(q[:, :ntr], dgr[...])
    iug[1] = SCALE * dot_tn(q[:, ntr:], dur[...])
    for h in range(2):
        finish(1, h, x_add)
    oug[...] = SCALE * dot_tn(qz, held[0, 1])
    idg[...] = SCALE * dot_tn(held[0, 0], wq)
    out = wts[e][:, :1] * back[0, pl.ds(0, tok), :].astype(F32)
    for m in range(1, ne):
        for h in range(2):
            zret[0, h, m].wait_recv()
        out = out + wts[flip(e, m)][:, :1] * home[0, m].astype(F32)
    mixed[...] = out.astype(BF16)
    grad = back[1, pl.ds(0, tok), :].astype(F32)
    for m in range(1, ne):
        for h in range(2):
            zret[1, h, m].wait_recv()
        grad = grad + home[1, m].astype(F32)
    igrad[...] = grad.astype(BF16)
    for c in pending:
        c.wait_send()


def output_kernel(*refs):
    n = (len(refs) - 1) // 2
    copies = [pltpu.make_async_copy(refs[i], refs[n + i], refs[-1].at[i]) for i in range(n)]
    for c in copies:
        c.start()
    for c in copies:
        c.wait()


def per_device(
    tokens, out_grad, expert_ids, tenant_ids, router_logits,
    gate_projection_weight, up_projection_weight, down_projection_weight,
    input_down_maps, input_up_maps, output_down_map, output_up_map,
):
    ne, nd, nf = lax.axis_size("expert"), lax.axis_size("dp"), lax.axis_size("ffn")
    tok, quarter = tokens.shape
    hidden = gate_projection_weight.shape[2]
    ntr = output_down_map.shape[2]
    rows_d = ne * tok
    rows = nd * rows_d
    routes = orders(nd, nf)
    rs_bufs = []
    for r in routes:
        dims = [r[-1]] + r[:-1]
        for i in range(1, len(dims)):
            rs_bufs.append(pltpu.VMEM((2, len(received(dims, i, nd, nf)), rows_d, quarter // 2), BF16))
    n1, n2 = max(len(bits_of(nf)), 1), len(routes[0])
    n_sem = 2 * (ne - 1) + nd + ne * n2 + 2 * nd * nf * max(1, ne // 2 if ne <= 4 else 1)
    n_sem += n1 + n2 + 2 * nf + 4 * nd * nf + 4 * (ne - 1)
    vmem = pl.BlockSpec(memory_space=pltpu.VMEM)
    hbm = pl.BlockSpec(memory_space=pl.ANY)
    outs = (
        jax.ShapeDtypeStruct(tokens.shape, BF16),
        jax.ShapeDtypeStruct(tokens.shape, BF16),
        jax.ShapeDtypeStruct(input_down_maps.shape[1:], F32),
        jax.ShapeDtypeStruct(input_up_maps.shape[1:], F32),
        jax.ShapeDtypeStruct(output_down_map.shape[1:], F32),
        jax.ShapeDtypeStruct(output_up_map.shape[1:], F32),
    )
    scratch = [
        pltpu.VMEM(tokens.shape, BF16),
        pltpu.VMEM(tokens.shape, BF16),
        pltpu.VMEM(expert_ids.shape[::-1], jnp.int32),
        pltpu.VMEM((1, tok), jnp.int32),
        pltpu.VMEM(router_logits.shape[::-1], F32),
        pltpu.VMEM(input_down_maps.shape[1:], BF16),
        pltpu.VMEM(input_up_maps.shape[1:], BF16),
        pltpu.VMEM(output_down_map.shape[1:], BF16),
        pltpu.VMEM(output_up_map.shape[1:], BF16),
        pltpu.VMEM((ne, 2, tok, quarter), BF16),
        pltpu.VMEM((ne, tok, ntr), F32),
        pltpu.VMEM((ne, tok, LANES), F32),
        pltpu.VMEM((nf, 2, rows, quarter), BF16),
        pltpu.VMEM((nd, rows_d, ntr), F32),
        pltpu.VMEM((nf, quarter, hidden), BF16),
        pltpu.VMEM((nf, quarter, hidden), BF16),
        pltpu.VMEM((nf, hidden, quarter), BF16),
        pltpu.VMEM((rows, hidden), F32),
        pltpu.VMEM((rows, hidden), F32),
        pltpu.VMEM((rows, hidden), F32),
        pltpu.VMEM((rows, hidden), BF16),
        pltpu.VMEM((rows, hidden), BF16),
        pltpu.VMEM((rows, hidden), BF16),
        pltpu.VMEM((2, nf, rows, quarter), BF16),
        pltpu.VMEM((2, nf // 2, rows, quarter), BF16),
        pltpu.VMEM((2, rows_d, quarter), BF16),
        pltpu.VMEM((2, ne, tok, quarter), BF16),
        pltpu.VMEM((n1, rows, LANES), F32),
        pltpu.VMEM((n1, rows, LANES), F32),
        pltpu.VMEM((n2, rows, LANES), F32),
        pltpu.VMEM((n2, rows, LANES), F32),
        *rs_bufs,
        pltpu.SemaphoreType.DMA((9,)),
        pltpu.SemaphoreType.DMA((3 * nf,)),
        pltpu.SemaphoreType.DMA((n_sem,)),
        pltpu.SemaphoreType.DMA((n_sem,)),
    ]
    limit = 54 if rows <= 64 else 60
    parts = pl.pallas_call(
        functools.partial(layer_kernel, nd, ne, nf, tok),
        out_shape=tuple(pltpu.VMEM(o.shape, o.dtype) for o in outs),
        in_specs=[hbm] * 12,
        out_specs=[vmem] * 6,
        scratch_shapes=scratch,
        compiler_params=pltpu.CompilerParams(
            collective_id=0, has_side_effects=True, vmem_limit_bytes=limit * MIB
        ),
    )(
        tokens, out_grad, expert_ids.T, tenant_ids.reshape(1, tok), router_logits.T,
        gate_projection_weight, up_projection_weight, down_projection_weight,
        input_down_maps, input_up_maps, output_down_map, output_up_map,
    )
    mixed, igrad, idg, iug, odg, oug = pl.pallas_call(
        output_kernel,
        out_shape=outs,
        in_specs=[vmem] * 6,
        out_specs=[hbm] * 6,
        scratch_shapes=[pltpu.SemaphoreType.DMA((6,))],
        compiler_params=pltpu.CompilerParams(vmem_limit_bytes=8 * 1024 * 1024),
    )(*parts)
    return mixed, igrad, idg[None], iug[None], odg[None], oug[None]


MIB = 1 << 20


def solution(mesh):
    return jax.shard_map(
        per_device,
        mesh=mesh,
        in_specs=(
            P(("dp", "expert"), "ffn"),
            P(("dp", "expert"), "ffn"),
            P(("dp", "expert"), None),
            P(("dp", "expert")),
            P(("dp", "expert"), None),
            P("expert", None, ("dp", "ffn")),
            P("expert", None, ("dp", "ffn")),
            P("expert", ("dp", "ffn"), None),
            P("expert", "ffn", None),
            P("expert", None, None, ("dp", "ffn")),
            P("expert", ("dp", "ffn"), None),
            P("expert", None, "ffn"),
        ),
        out_specs=(
            P(("dp", "expert"), "ffn"),
            P(("dp", "expert"), "ffn"),
            P("expert", "ffn", None),
            P("expert", None, None, ("dp", "ffn")),
            P("expert", ("dp", "ffn"), None),
            P("expert", None, "ffn"),
        ),
        check_vma=False,
    )
```
